32 devices in a mesh: node: 16 (over z, x, core), head: 2 (over y).
Axes of the slice: x: 2, y: 2, z: 4, core: 2. Of those that a mesh axis runs over, the one named last changes fastest.
Arguments:
- features: bfloat16 [32768, 100], P('node'), may hold values from -6 to 6
- proj_weight: bfloat16 [100, 512], P(None, 'head'), may hold values from -0.625 to 0.625
- score_src: float32 [8, 64], P('head'), may hold values from -150 to 150
- score_dst: float32 [8, 64], P('head'), may hold values from -0.75 to 0.75
- request_rows: int32 [16, 16, 512], P('node'), may hold values from 0 to 2047
- slot_index: int32 [8192, 16], P('node'), may hold values from 0 to 8191
- slot_count: int32 [8192], P('node'), may hold values from 1 to 16
- out_weight: bfloat16 [512, 512], replicated, may hold values from -0.25 to 0.25
Outputs:
- layer_out: bfloat16 [8192, 512], P(('node', 'head'))
The draws below stay inside these ranges and needn't reach their ends.
All inputs are finite; a program needn't handle non-finite values.
Results may differ from the reference program's by a relative error of at most 0.012.
The reference program's roundings to bfloat16 on the way count: a program that leaves them out, or rounds other values in their place, can miss the bound.
Values may be sent and summed in bfloat16 or wider, within the bound.
A program may use at most 64 MiB of HBM per device.

```python
import math
import jax
import jax.numpy as jnp
import numpy as np
from jax import lax

FEAT = 100
HEADS = 8
HEAD_DIM = 64
D_OUT = 512
SLOTS = 16
NODE_DEV = 2048
DST_DEV = 512
CAP = 512
NODES = 32768
DESTS = 8192
N_NODE = 16


def draw_score_src(key, part):
    base = jax.random.normal(jax.random.fold_in(key, 11), (HEADS, HEAD_DIM), jnp.float32)
    base = jnp.clip(base, -4.0, 4.0) / math.sqrt(HEAD_DIM)
    return jnp.clip(base, -150.0, 150.0)


def plant(values, rng, least, high):
    longest = values.shape.index(max(values.shape))
    spots = []
    for shift in (0, 1):
        where = [jax.random.randint(jax.random.fold_in(rng, axis), (), 0, length) for axis, length in enumerate(values.shape)]
        where[longest] = (where[longest] + shift) % values.shape[longest]
        spots.append(tuple(where))
    return values.at[spots[0]].set(least).at[spots[1]].set(high)


def block_scale(stream_key, shape, shards, low, largest):
    level = 1.0
    for position, parts in shards:
        heights = jax.random.uniform(jax.random.fold_in(jax.random.fold_in(stream_key, 6), position), (parts,), jnp.float32, low / len(shards), largest / len(shards))
        level = level * jnp.repeat(jnp.exp(heights), shape[position] // parts).reshape((-1,) + (1,) * (len(shape) - 1 - position))
    return level


def cumulative_ranks(amount, slope):
    weights = [(1 << 20) // math.isqrt(standing ** slope) + 1 for standing in range(1, amount + 1)]
    spread = 1 + sum(weights) // (1 << 30)
    return np.cumsum(np.array([max(1, weight // spread) for weight in weights]))


def ranked(key, shape, number_of, skew):
    table = cumulative_ranks(number_of, skew)
    ticket = jax.random.randint(jax.random.fold_in(key, 1), shape, 0, int(table[number_of - 1]))
    standing = jnp.searchsorted(jnp.asarray(table, jnp.int32), ticket, side="right")
    return jax.random.permutation(jax.random.fold_in(key, 2), number_of)[standing].astype(jnp.int32)


def gaussian(key, shape, deviation, bound, pieces=(), kind=jnp.bfloat16):
    values = jax.random.normal(key, shape, jnp.float32) * deviation
    if len(pieces) > 0:
        values = block_scale(key, shape, pieces, -0.22, 0.18) * values
    return jnp.clip(values, min=-bound, max=bound).astype(kind)


def setup_inputs(seed: int = 0) -> dict:
    key_of = jax.random.split(jax.random.key(seed), 9)
    return {
        "features": gaussian(key_of[0], (NODES, FEAT), 1.0, 6.0, ((0, 16),)),
        "proj_weight": gaussian(key_of[1], (FEAT, HEADS * HEAD_DIM), FEAT ** -0.5, 0.625, ((1, 2),)),
        "score_src": draw_score_src(jax.random.fold_in(key_of[8], 71), 0),
        "score_dst": gaussian(key_of[3], (HEADS, HEAD_DIM), HEAD_DIM ** -0.5, 0.75, ((0, 2),), jnp.float32),
        "request_rows": plant(jax.random.randint(key_of[4], (N_NODE, N_NODE, CAP), 0, NODE_DEV), jax.random.fold_in(key_of[4], 1), 0, NODE_DEV - 1).astype(jnp.int32),
        "slot_index": plant(ranked(key_of[5], (DESTS, SLOTS), N_NODE * CAP, 1), jax.random.fold_in(key_of[5], 3), 0, (N_NODE * CAP) - 1).astype(jnp.int32),
        "slot_count": plant(jax.random.randint(key_of[6], (DESTS,), 1, SLOTS + 1), jax.random.fold_in(key_of[6], 1), 1, SLOTS).astype(jnp.int32),
        "out_weight": gaussian(key_of[7], (HEADS * HEAD_DIM, D_OUT), (HEADS * HEAD_DIM) ** -0.5, 0.25),
    }


def reference(features, proj_weight, score_src, score_dst, request_rows, slot_index, slot_count, out_weight):
    flat_requests = request_rows.reshape(N_NODE, N_NODE * CAP)
    owner_dev = (slot_index // CAP).astype(jnp.int32)
    device_of = (jnp.arange(DESTS, dtype=jnp.int32) // DST_DEV).astype(jnp.int32)
    local_row = flat_requests[device_of[:, None], slot_index]
    neighbour = (owner_dev * NODE_DEV + local_row).astype(jnp.int32)

    def one_block(pair):
        ids, counts = pair
        picked = features[ids.reshape(-1)]
        zvals = jnp.dot(picked, proj_weight, preferred_element_type=jnp.float32).astype(jnp.bfloat16)
        zfloat = zvals.astype(jnp.float32).reshape(DST_DEV, SLOTS, HEADS, HEAD_DIM)
        src_part = jnp.einsum("rshd,hd->rsh", zfloat, score_src.astype(jnp.float32))
        dst_part = jnp.einsum("rhd,hd->rh", zfloat[:, 0], score_dst.astype(jnp.float32))
        logit = src_part + dst_part[:, None, :]
        logit = jnp.where(logit > 0, logit, 0.2 * logit)
        live_mask = (jnp.arange(SLOTS, dtype=jnp.int32)[None, :] < counts[:, None])[:, :, None]
        logit = jnp.where(live_mask, logit, -1e30)
        peak = jnp.max(logit, axis=1, keepdims=True)
        weights = jnp.where(live_mask, jnp.exp(logit - peak), 0.0)
        alpha = (weights / jnp.sum(weights, axis=1, keepdims=True)).astype(jnp.bfloat16)
        summed = jnp.einsum("rsh,rshd->rhd", alpha.astype(jnp.float32), zfloat)
        hidden = jax.nn.elu(summed).astype(jnp.bfloat16).reshape(DST_DEV, HEADS * HEAD_DIM)
        return jnp.dot(hidden, out_weight, preferred_element_type=jnp.float32).astype(jnp.bfloat16)

    result = lax.map(one_block, (neighbour.reshape(N_NODE, DST_DEV, SLOTS), slot_count.reshape(N_NODE, DST_DEV)))
    return result.reshape(DESTS, D_OUT)
```

```python
import functools

import jax
import jax.numpy as jnp
from jax import lax
from jax.experimental import pallas as pl
from jax.experimental.pallas import tpu as pltpu
from jax.sharding import PartitionSpec as P

LANES = 128


def quotient(value, divisor):
    if divisor & (divisor - 1) == 0:
        return lax.shift_right_logical(value, divisor.bit_length() - 1)
    return lax.div(value, divisor)


def elu(x):
    series = x * (1.0 + x * (0.5 + x * (1 / 6 + x * (1 / 24 + x * (1 / 120)))))
    below = jnp.where(x > -0.1, series, jnp.exp(jnp.minimum(x, 0.0)) - 1.0)
    return jnp.where(x > 0, x, below)


def address_rows(slot_ref, request_ref, where_ref, owned, capacity):
    unroll = 16

    def body(step, carry):
        for k in range(unroll):
            place = step * unroll + k
            b = slot_ref[place]
            where_ref[place] = quotient(b, capacity) * owned + request_ref[b]
        return carry

    lax.fori_loop(0, where_ref.shape[0] // unroll, body, 0)


def gather_rows(where_ref, table_ref, picked_ref):
    unroll = 64

    def body(step, carry):
        base = pl.multiple_of(step * unroll, unroll)
        for k in range(unroll):
            picked_ref[pl.ds(base + k, 1), :] = table_ref[pl.ds(where_ref[base + k], 1), :]
        return carry

    lax.fori_loop(0, picked_ref.shape[0] // unroll, body, 0)


def score_matrix(row, heads, head_dim):
    width = row.shape[1]
    hi = row.astype(jnp.bfloat16).astype(jnp.float32)
    mid = (row - hi).astype(jnp.bfloat16).astype(jnp.float32)
    lo = row - hi - mid
    at = lax.broadcasted_iota(jnp.int32, (LANES, width), 0)
    head_of = quotient(lax.broadcasted_iota(jnp.int32, (LANES, width), 1), head_dim)
    total = jnp.zeros((LANES, width), jnp.float32)
    for place, term in enumerate((hi, mid, lo)):
        total = jnp.where(at == head_of + place * heads, term, total)
    return total.astype(jnp.bfloat16)


def scores(zvals, matrix, heads):
    parts = lax.dot_general(
        zvals, matrix, (((1,), (1,)), ((), ())), preferred_element_type=jnp.float32
    )
    return parts + (
        pltpu.roll(parts, LANES - heads, 1) + pltpu.roll(parts, LANES - 2 * heads, 1)
    )


def attend(heads, weights_ref, count_ref, out_weight_ref, out_ref, picked_ref, z_ref, logit_ref):
    rows, width = out_ref.shape[0], out_weight_ref.shape[0]
    feat = picked_ref.shape[1]
    slots = z_ref.shape[0]
    head_dim = width // heads
    proj = weights_ref[0:feat, :].astype(jnp.bfloat16)
    src = score_matrix(weights_ref[feat : feat + 1, :], heads, head_dim)
    dst = score_matrix(weights_ref[feat + 1 : feat + 2, :], heads, head_dim)
    spread = (
        lax.broadcasted_iota(jnp.int32, (LANES, width), 0)
        == quotient(lax.broadcasted_iota(jnp.int32, (LANES, width), 1), head_dim)
    ).astype(jnp.bfloat16)

    def project(s):
        picked = picked_ref[pl.ds(pl.multiple_of(s * rows, rows), rows), :].astype(jnp.bfloat16)
        z = jnp.dot(picked, proj, preferred_element_type=jnp.float32).astype(jnp.bfloat16)
        z_ref[s] = z
        return z

    z0 = project(0)
    dst_part = scores(z0, dst, heads)
    count = count_ref[...]

    def logits(s, peak):
        z = project(s)
        logit = scores(z, src, heads) + dst_part
        logit = jnp.where(logit > 0, logit, 0.2 * logit)
        logit = jnp.where(s < count, logit, -1e30)
        logit_ref[s] = logit
        return jnp.maximum(peak, logit)

    peak = lax.fori_loop(0, slots, logits, jnp.full((rows, LANES), -1e30, jnp.float32))

    def weigh(s, total):
        weight = jnp.where(s < count, jnp.exp(logit_ref[s] - peak), 0.0)
        logit_ref[s] = weight
        return total + weight

    total = lax.fori_loop(0, slots, weigh, jnp.zeros((rows, LANES), jnp.float32))
    inverse = 1.0 / total

    def combine(s, summed):
        alpha = (logit_ref[s] * inverse).astype(jnp.bfloat16)
        wide = jnp.dot(alpha, spread, preferred_element_type=jnp.float32)
        return summed + wide * z_ref[s].astype(jnp.float32)

    summed = lax.fori_loop(0, slots, combine, jnp.zeros((rows, width), jnp.float32))
    hidden = elu(summed).astype(jnp.bfloat16)
    out_ref[...] = jnp.dot(
        hidden, out_weight_ref[...], preferred_element_type=jnp.float32
    ).astype(jnp.bfloat16)


def kernel(
    owned,
    capacity,
    heads,
    chunks,
    slot_ref,
    request_ref,
    weights_ref,
    count_ref,
    out_weight_ref,
    nodes_ref,
    out_ref,
    where_ref,
    landing_ref,
    table_ref,
    picked_ref,
    z_ref,
    logit_ref,
    sems,
):
    rows = nodes_ref.shape[0] // chunks
    copies = []
    for c in range(chunks):
        part = pl.ds(c * rows, rows)
        copies.append(
            pltpu.make_async_copy(nodes_ref.at[part, :], landing_ref.at[part, :], sems.at[c])
        )
        copies[-1].start()
    address_rows(slot_ref, request_ref, where_ref, owned, capacity)
    for c in range(chunks):
        copies[c].wait()
        block = 256

        def widen(step, carry):
            part = pl.ds(pl.multiple_of(c * rows + step * block, block), block)
            table_ref[part, :] = landing_ref[part, :].astype(jnp.float32)
            return carry

        lax.fori_loop(0, rows // block, widen, 0)
    gather_rows(where_ref, table_ref, picked_ref)
    attend(heads, weights_ref, count_ref, out_weight_ref, out_ref, picked_ref, z_ref, logit_ref)


def local(
    features, proj_weight, score_src, score_dst, request_rows, slot_index, slot_count, out_weight
):
    planes = lax.axis_size("head")
    groups = lax.axis_size("node")
    plane = lax.axis_index("head")
    owned, feat = features.shape
    capacity = request_rows.shape[2]
    heads = score_src.shape[0] * planes
    width = proj_weight.shape[1]
    dst_rows = slot_index.shape[0] // planes
    slots = slot_index.shape[1]

    share = lax.dynamic_slice_in_dim(features, plane * (owned // planes), owned // planes, 0)
    nodes = lax.all_gather(share, ("node", "head"), axis=0, tiled=True)
    mine = jnp.concatenate(
        [
            proj_weight.astype(jnp.float32),
            score_src.reshape(1, width),
            score_dst.reshape(1, width),
        ],
        axis=0,
    )
    weights = lax.all_gather(mine, "head", axis=1, tiled=True)
    slot = lax.dynamic_slice_in_dim(slot_index, plane * dst_rows, dst_rows, 0).T.reshape(-1)
    count = jnp.broadcast_to(
        lax.dynamic_slice_in_dim(slot_count, plane * dst_rows, dst_rows, 0)[:, None],
        (dst_rows, LANES),
    )
    total_nodes = groups * owned
    vmem = pl.BlockSpec(memory_space=pltpu.VMEM)
    smem = pl.BlockSpec(memory_space=pltpu.SMEM)
    chunks = 8
    return pl.pallas_call(
        functools.partial(kernel, owned, capacity, heads, chunks),
        out_shape=jax.ShapeDtypeStruct((dst_rows, out_weight.shape[1]), jnp.bfloat16),
        in_specs=[smem, smem, vmem, vmem, vmem, pl.BlockSpec(memory_space=pl.ANY)],
        out_specs=vmem,
        scratch_shapes=[
            pltpu.SMEM((dst_rows * slots,), jnp.int32),
            pltpu.VMEM((total_nodes, feat), jnp.bfloat16),
            pltpu.VMEM((total_nodes, feat), jnp.float32),
            pltpu.VMEM((dst_rows * slots, feat), jnp.float32),
            pltpu.VMEM((slots, dst_rows, width * planes), jnp.bfloat16),
            pltpu.VMEM((slots, dst_rows, LANES), jnp.float32),
            pltpu.SemaphoreType.DMA((chunks,)),
        ],
        compiler_params=pltpu.CompilerParams(vmem_limit_bytes=67043328),
    )(slot, request_rows.reshape(-1), weights, count, out_weight, nodes)


def solution(mesh):
    in_specs = (
        P("node", None),
        P(None, "head"),
        P("head", None),
        P("head", None),
        P("node", None, None),
        P("node", None),
        P("node"),
        P(),
    )
    out_specs = P(("node", "head"), None)
    return jax.shard_map(local, mesh=mesh, in_specs=in_specs, out_specs=out_specs, check_vma=False)
```

```python
import functools

import jax
import jax.numpy as jnp
from jax import lax
from jax.experimental import pallas as pl
from jax.experimental.pallas import tpu as pltpu
from jax.sharding import PartitionSpec as P

LANES = 128


def quotient(value, divisor):
    if divisor & (divisor - 1) == 0:
        return lax.shift_right_logical(value, divisor.bit_length() - 1)
    return lax.div(value, divisor)


def elu(x):
    series = x * (1.0 + x * (0.5 + x * (1 / 6 + x * (1 / 24 + x * (1 / 120)))))
    below = jnp.where(x > -0.1, series, jnp.exp(jnp.minimum(x, 0.0)) - 1.0)
    return jnp.where(x > 0, x, below)


def address_rows(first, amount, base, slots, dst_rows, slot_ref, request_ref, where_ref, owned, capacity):
    def body(row, carry):
        for k in range(slots):
            b = slot_ref[base + row, k]
            owner = quotient(b, capacity)
            where_ref[k * dst_rows + row] = owner * owned + request_ref[0, owner, b - owner * capacity]
        return carry

    lax.fori_loop(first, first + amount, body, 0)


def gather_rows(where_ref, table_ref, picked_ref):
    unroll = 64

    def body(step, carry):
        base = pl.multiple_of(step * unroll, unroll)
        for k in range(unroll):
            picked_ref[pl.ds(base + k, 1), :] = table_ref[pl.ds(where_ref[base + k], 1), :]
        return carry

    lax.fori_loop(0, picked_ref.shape[0] // unroll, body, 0)


def score_matrix(score_ref, heads, head_dim):
    table = jnp.concatenate([score_ref[p] for p in range(score_ref.shape[0])], axis=0)
    wide = jnp.concatenate([table] * heads, axis=1)
    shape = (heads, heads * head_dim)
    head_of = quotient(lax.broadcasted_iota(jnp.int32, shape, 1), head_dim)
    row = jnp.where(head_of == lax.broadcasted_iota(jnp.int32, shape, 0), wide, 0.0)
    hi = row.astype(jnp.bfloat16).astype(jnp.float32)
    mid = (row - hi).astype(jnp.bfloat16).astype(jnp.float32)
    lo = row - hi - mid
    rest = jnp.zeros((LANES - 3 * heads, heads * head_dim), jnp.float32)
    return jnp.concatenate([hi, mid, lo, rest], axis=0).astype(jnp.bfloat16)


def scores(zvals, matrix, heads):
    parts = lax.dot_general(
        zvals, matrix, (((1,), (1,)), ((), ())), preferred_element_type=jnp.float32
    )
    return parts + (
        pltpu.roll(parts, LANES - heads, 1) + pltpu.roll(parts, LANES - 2 * heads, 1)
    )


def attend(heads, proj_ref, src_ref, dst_ref, count_ref, out_weight_ref, out_ref, picked_ref, z_ref, logit_ref):
    rows, width = out_ref.shape[0], out_weight_ref.shape[0]
    feat = picked_ref.shape[1]
    slots = z_ref.shape[0]
    head_dim = width // heads
    proj = jnp.concatenate([proj_ref[p] for p in range(proj_ref.shape[0])], axis=1)
    src = score_matrix(src_ref, heads, head_dim)
    dst = score_matrix(dst_ref, heads, head_dim)
    spread = (
        lax.broadcasted_iota(jnp.int32, (LANES, width), 0)
        == quotient(lax.broadcasted_iota(jnp.int32, (LANES, width), 1), head_dim)
    ).astype(jnp.bfloat16)

    def project(s):
        picked = picked_ref[pl.ds(pl.multiple_of(s * rows, rows), rows), :].astype(jnp.bfloat16)
        z = jnp.dot(picked, proj, preferred_element_type=jnp.float32).astype(jnp.bfloat16)
        z_ref[s] = z
        return z

    z0 = project(0)
    dst_part = scores(z0, dst, heads)
    count = count_ref[...]

    def logits(s, peak):
        z = project(s)
        logit = scores(z, src, heads) + dst_part
        logit = jnp.where(logit > 0, logit, 0.2 * logit)
        logit = jnp.where(s < count, logit, -1e30)
        logit_ref[s] = logit
        return jnp.maximum(peak, logit)

    peak = lax.fori_loop(0, slots, logits, jnp.full((rows, LANES), -1e30, jnp.float32))

    def weigh(s, total):
        weight = jnp.where(s < count, jnp.exp(logit_ref[s] - peak), 0.0)
        logit_ref[s] = weight
        return total + weight

    total = lax.fori_loop(0, slots, weigh, jnp.zeros((rows, LANES), jnp.float32))
    inverse = 1.0 / total

    def combine(s, summed):
        alpha = (logit_ref[s] * inverse).astype(jnp.bfloat16)
        wide = jnp.dot(alpha, spread, preferred_element_type=jnp.float32)
        return summed + wide * z_ref[s].astype(jnp.float32)

    summed = lax.fori_loop(0, slots, combine, jnp.zeros((rows, width), jnp.float32))
    hidden = elu(summed).astype(jnp.bfloat16)
    out_ref[...] = jnp.dot(
        hidden, out_weight_ref[...], preferred_element_type=jnp.float32
    ).astype(jnp.bfloat16)


def plan(lines, cores, planes, groups, pieces):
    far = ([1, lines - 1] + list(range(2, lines - 1)))[: lines - 1]
    second, last = [], []
    first = [("z", d, 0, 0, s) for s in range(pieces) for d in far]
    own = [("o", 0, dx, dy, s) for dy in range(planes) for s in range(pieces) for dx in range(1, groups)]
    merged = []
    while first or own:
        merged += first[:2] + own[:1]
        first, own = first[2:], own[1:]
    for s in range(pieces):
        for d in far:
            for dy in range(1, planes):
                second.append(("y", d, 0, dy, s))
        for d in far:
            for dx in range(1, groups):
                second.append(("x", d, dx, 0, s))
    for s in range(pieces):
        for d in far:
            for dx in range(1, groups):
                for dy in range(1, planes):
                    last.append(("d", d, dx, dy, s))
    return far, merged + second + last


def kernel(
    lines,
    groups,
    cores,
    planes,
    pieces,
    capacity,
    heads,
    slot_ref,
    request_ref,
    slot_count_ref,
    proj_in,
    src_in,
    dst_in,
    out_weight_ref,
    nodes_ref,
    out_ref,
    where_ref,
    landing_ref,
    table_ref,
    picked_ref,
    z_ref,
    logit_ref,
    count_ref,
    proj_ref,
    src_ref,
    dst_ref,
    local_sems,
    send_sems,
    recv_sems,
    weight_sems,
):
    owned = nodes_ref.shape[0]
    unit = owned // planes
    piece = unit // pieces
    dst_rows = out_ref.shape[0]
    slots = z_ref.shape[0]
    node, y = lax.axis_index("node"), lax.axis_index("head")
    z = node // (groups * cores)
    x = (node // cores) % groups
    c = node % cores

    def device(dz, dx, dc, dy):
        place = (((z + dz) % lines) * groups + (x + dx) % groups) * cores + (c + dc) % cores
        return {"node": place, "head": (y + dy) % planes}

    def number(dz, dx, dc, dy, s):
        place = (((z + dz) % lines) * groups + (x + dx) % groups) * cores + (c + dc) % cores
        return (place * planes + (y + dy) % planes) * pieces + s

    def part(index):
        return pl.ds(pl.multiple_of(index * piece, piece), piece)

    far, events = plan(lines, cores, planes, groups, pieces)
    peers = [(d, 0, 0, 0) for d in far]
    peers += [(0, d, 0, 0) for d in range(1, groups)]
    peers += [(0, 0, d, 0) for d in range(1, cores)]
    peers += [(0, 0, 0, d) for d in range(1, planes)]
    barrier = pltpu.get_barrier_semaphore()
    for peer in peers:
        pl.semaphore_signal(barrier, inc=1, device_id=device(*peer))
    own_rows = pl.ds(pl.multiple_of(node * owned, owned), owned)
    fetch = [pltpu.make_async_copy(nodes_ref, landing_ref.at[own_rows, :], local_sems.at[0])]
    fetch += [
        pltpu.make_async_copy(given, held.at[y], local_sems.at[1 + i])
        for i, (given, held) in enumerate(((proj_in, proj_ref), (src_in, src_ref), (dst_in, dst_ref)))
    ]
    for copy in fetch:
        copy.start()
    pl.semaphore_wait(barrier, len(peers))
    for copy in fetch:
        copy.wait()

    sent = []

    def send(index, peer):
        view = landing_ref.at[part(index), :]
        copy = pltpu.make_async_remote_copy(
            src_ref=view,
            dst_ref=view,
            send_sem=send_sems.at[len(sent)],
            recv_sem=recv_sems.at[index],
            device_id=device(*peer),
        )
        copy.start()
        sent.append(copy)

    def landed(index):
        view = landing_ref.at[part(index), :]
        pltpu.make_async_remote_copy(
            src_ref=view,
            dst_ref=view,
            send_sem=send_sems.at[0],
            recv_sem=recv_sems.at[index],
            device_id=device(*peers[0]),
        ).wait_recv()

    block = 128 if piece % 128 == 0 else piece

    def widen(index):
        def body(step, carry):
            rows = pl.ds(pl.multiple_of(index * piece + step * block, block), block)
            table_ref[rows, :] = landing_ref[rows, :].astype(jnp.float32)
            return carry

        lax.fori_loop(0, piece // block, body, 0)

    for s in range(pieces):
        for d in far:
            send(number(0, 0, 0, 0, s), (d, 0, 0, 0))
    for dy in range(planes):
        for s in range(pieces):
            for dx in range(1, groups):
                send(number(0, 0, 0, dy, s), (0, dx, 0, 0))
    shared = []
    for i, held in enumerate((proj_ref, src_ref, dst_ref)):
        for dy in range(1, planes):
            copy = pltpu.make_async_remote_copy(
                src_ref=held.at[y],
                dst_ref=held.at[y],
                send_sem=weight_sems.at[0, i, dy],
                recv_sem=weight_sems.at[1, i, dy],
                device_id=device(0, 0, 0, dy),
            )
            copy.start()
            shared.append(copy)
    for dy in range(planes):
        for s in range(pieces):
            for dc in range(1, cores):
                send(number(0, 0, 0, dy, s), (0, 0, dc, 0))

    late = far[:1]
    todo = []
    steps = 16 if dst_rows % 16 == 0 else 1
    share = dst_rows // steps
    base = y * dst_rows

    def catch_up(keep):
        while len(todo) > keep:
            dz, dx, dy, s = todo.pop(0)
            for dc in range(1, cores):
                index = number(dz, dx, dc, dy, s)
                landed(index)
                widen(index)

    for dy in range(planes):
        for s in range(pieces):
            widen(number(0, 0, 0, dy, s))
            todo.append((0, 0, dy, s))
    for e, (kind, dz, dx, dy, s) in enumerate(events):
        if e < steps:
            address_rows(
                e * share, share, base, slots, dst_rows, slot_ref, request_ref, where_ref, owned, capacity
            )
        if e == steps:

            def fill(row, carry):
                count_ref[pl.ds(row, 1), :] = jnp.full((1, LANES), slot_count_ref[base + row])
                return carry

            lax.fori_loop(0, dst_rows, fill, 0)
        index = number(dz, dx, 0, dy, s)
        landed(index)
        if kind == "z":
            for d in range(1, planes):
                send(index, (0, 0, 0, d))
        if kind == "z" or (kind == "y" and dz in late):
            for d in range(1, groups):
                send(index, (0, d, 0, 0))
        if kind == "x" and dz not in late:
            for d in range(1, planes):
                send(index, (0, 0, 0, d))
        for dc in range(1, cores):
            send(index, (0, 0, dc, 0))
        widen(index)
        todo.append((dz, dx, dy, s))
        catch_up(2)
    catch_up(0)
    for copy in sent:
        copy.wait_send()
    for copy in shared:
        copy.wait()
    gather_rows(where_ref, table_ref, picked_ref)
    attend(
        heads, proj_ref, src_ref, dst_ref, count_ref, out_weight_ref, out_ref, picked_ref, z_ref, logit_ref
    )


def local(
    features, proj_weight, score_src, score_dst, request_rows, slot_index, slot_count, out_weight
):
    planes = lax.axis_size("head")
    nodes = lax.axis_size("node")
    owned, feat = features.shape
    capacity = request_rows.shape[2]
    local_heads, head_dim = score_src.shape
    heads = local_heads * planes
    width = proj_weight.shape[1]
    dst_rows = slot_index.shape[0] // planes
    slots = slot_index.shape[1]
    cores = 2 if nodes % 2 == 0 else 1
    chips = nodes // cores
    lines = 4 if chips % 4 == 0 else chips
    groups = chips // lines
    pieces = 2 if planes <= 2 else 1
    units = nodes * planes * pieces
    vmem = pl.BlockSpec(memory_space=pltpu.VMEM)
    smem = pl.BlockSpec(memory_space=pltpu.SMEM)
    anyway = pl.BlockSpec(memory_space=pl.ANY)
    far, events = plan(lines, cores, planes, groups, pieces)
    sends = pieces * (len(far) + planes * (groups - 1) + planes * (cores - 1))
    for kind, dz, _, _, _ in events:
        sends += cores - 1
        if kind == "z":
            sends += planes - 1 + groups - 1
        if kind == "y" and dz in far[:1]:
            sends += groups - 1
        if kind == "x" and dz not in far[:1]:
            sends += planes - 1
    return pl.pallas_call(
        functools.partial(kernel, lines, groups, cores, planes, pieces, capacity, heads),
        out_shape=jax.ShapeDtypeStruct((dst_rows, out_weight.shape[1]), jnp.bfloat16),
        in_specs=[smem, smem, smem, anyway, anyway, anyway, vmem, anyway],
        out_specs=vmem,
        scratch_shapes=[
            pltpu.SMEM((dst_rows * slots,), jnp.int32),
            pltpu.VMEM((nodes * owned, feat), jnp.bfloat16),
            pltpu.VMEM((nodes * owned, feat), jnp.float32),
            pltpu.VMEM((dst_rows * slots, feat), jnp.float32),
            pltpu.VMEM((slots, dst_rows, width * planes), jnp.bfloat16),
            pltpu.VMEM((slots, dst_rows, LANES), jnp.float32),
            pltpu.VMEM((dst_rows, LANES), jnp.int32),
            pltpu.VMEM((planes, feat, width), jnp.bfloat16),
            pltpu.VMEM((planes, local_heads, head_dim), jnp.float32),
            pltpu.VMEM((planes, local_heads, head_dim), jnp.float32),
            pltpu.SemaphoreType.DMA((4,)),
            pltpu.SemaphoreType.DMA((sends,)),
            pltpu.SemaphoreType.DMA((units,)),
            pltpu.SemaphoreType.DMA((2, 3, planes)),
        ],
        compiler_params=pltpu.CompilerParams(
            vmem_limit_bytes=67043328, collective_id=0, has_side_effects=True
        ),
    )(slot_index, request_rows, slot_count, proj_weight, score_src, score_dst, out_weight, features)


def solution(mesh):
    in_specs = (
        P("node", None),
        P(None, "head"),
        P("head", None),
        P("head", None),
        P("node", None, None),
        P("node", None),
        P("node"),
        P(),
    )
    out_specs = P(("node", "head"), None)
    return jax.shard_map(local, mesh=mesh, in_specs=in_specs, out_specs=out_specs, check_vma=False)
```

```python
import functools
import math

import jax
import jax.numpy as jnp
from jax import lax
from jax.experimental import pallas as pl
from jax.experimental.pallas import tpu as pltpu
from jax.sharding import PartitionSpec as P

LANES = 128


def quotient(value, divisor):
    if divisor & (divisor - 1) == 0:
        return lax.shift_right_logical(value, divisor.bit_length() - 1)
    return lax.div(value, divisor)


def elu(x):
    series = x * (1.0 + x * (0.5 + x * (1 / 6 + x * (1 / 24 + x * (1 / 120)))))
    below = jnp.where(x > -0.1, series, jnp.exp(jnp.minimum(x, 0.0)) - 1.0)
    return jnp.where(x > 0, x, below)


def address_rows(first, amount, base, slots, dst_rows, slot_ref, request_ref, where_ref, owned, capacity):
    def body(row, carry):
        for k in range(slots):
            b = slot_ref[k, base + row]
            owner = quotient(b, capacity)
            where_ref[k * dst_rows + row] = owner * owned + request_ref[0, owner, b - owner * capacity]
        return carry

    lax.fori_loop(first, first + amount, body, 0)


def gather_rows(where_ref, table_ref, picked_ref):
    unroll = 64

    def body(step, carry):
        base = pl.multiple_of(step * unroll, unroll)
        for k in range(unroll):
            picked_ref[pl.ds(base + k, 1), :] = table_ref[pl.ds(where_ref[base + k], 1), :]
        return carry

    lax.fori_loop(0, picked_ref.shape[0] // unroll, body, 0)


def score_matrix(score_ref, heads, head_dim):
    table = jnp.concatenate([score_ref[p] for p in range(score_ref.shape[0])], axis=0)
    wide = jnp.concatenate([table] * heads, axis=1)
    shape = (heads, heads * head_dim)
    head_of = quotient(lax.broadcasted_iota(jnp.int32, shape, 1), head_dim)
    row = jnp.where(head_of == lax.broadcasted_iota(jnp.int32, shape, 0), wide, 0.0)
    hi = row.astype(jnp.bfloat16).astype(jnp.float32)
    mid = (row - hi).astype(jnp.bfloat16).astype(jnp.float32)
    lo = row - hi - mid
    rest = jnp.zeros((LANES - 3 * heads, heads * head_dim), jnp.float32)
    return jnp.concatenate([hi, mid, lo, rest], axis=0).astype(jnp.bfloat16)


def scores(zvals, matrix, heads):
    parts = lax.dot_general(
        zvals, matrix, (((1,), (1,)), ((), ())), preferred_element_type=jnp.float32
    )
    return parts + (
        pltpu.roll(parts, LANES - heads, 1) + pltpu.roll(parts, LANES - 2 * heads, 1)
    )


def attend(heads, proj_ref, src_ref, dst_ref, count_ref, out_weight_ref, out_ref, picked_ref, z_ref, logit_ref):
    rows, width = out_ref.shape[0], out_weight_ref.shape[0]
    feat = picked_ref.shape[1]
    slots = z_ref.shape[0]
    head_dim = width // heads
    proj = jnp.concatenate([proj_ref[p] for p in range(proj_ref.shape[0])], axis=1)
    src = score_matrix(src_ref, heads, head_dim)
    dst = score_matrix(dst_ref, heads, head_dim)
    spread = (
        lax.broadcasted_iota(jnp.int32, (LANES, width), 0)
        == quotient(lax.broadcasted_iota(jnp.int32, (LANES, width), 1), head_dim)
    ).astype(jnp.bfloat16)

    def project(s):
        picked = picked_ref[pl.ds(pl.multiple_of(s * rows, rows), rows), :].astype(jnp.bfloat16)
        z = jnp.dot(picked, proj, preferred_element_type=jnp.float32).astype(jnp.bfloat16)
        z_ref[s] = z
        return z

    z0 = project(0)
    dst_part = scores(z0, dst, heads)
    count = count_ref[...]

    def logits(s, peak):
        z = project(s)
        logit = scores(z, src, heads) + dst_part
        logit = jnp.where(logit > 0, logit, 0.2 * logit)
        logit = jnp.where(s < count, logit, -1e30)
        logit_ref[s] = logit
        return jnp.maximum(peak, logit)

    peak = lax.fori_loop(0, slots, logits, jnp.full((rows, LANES), -1e30, jnp.float32), unroll=True)

    def weigh(s, total):
        weight = jnp.where(s < count, jnp.exp(logit_ref[s] - peak), 0.0)
        logit_ref[s] = weight
        return total + weight

    total = lax.fori_loop(0, slots, weigh, jnp.zeros((rows, LANES), jnp.float32), unroll=True)
    inverse = 1.0 / total

    def combine(s, summed):
        alpha = (logit_ref[s] * inverse).astype(jnp.bfloat16)
        wide = jnp.dot(alpha, spread, preferred_element_type=jnp.float32)
        return summed + wide * z_ref[s].astype(jnp.float32)

    summed = lax.fori_loop(0, slots, combine, jnp.zeros((rows, width), jnp.float32), unroll=True)
    hidden = elu(summed).astype(jnp.bfloat16)
    out_ref[...] = jnp.dot(
        hidden, out_weight_ref[...], preferred_element_type=jnp.float32
    ).astype(jnp.bfloat16)


def plan(lines, cores, planes, groups, pieces):
    far = ([1, lines - 1] + list(range(2, lines - 1)))[: lines - 1]
    second, last = [], []
    first = [("z", d, 0, 0, s) for s in range(pieces) for d in far]
    own = [("o", 0, dx, dy, s) for dy in range(planes) for s in range(pieces) for dx in range(1, groups)]
    merged = []
    while first or own:
        merged += first[:2] + own[:1]
        first, own = first[2:], own[1:]
    for s in range(pieces):
        for d in far:
            for dy in range(1, planes):
                second.append(("y", d, 0, dy, s))
        for d in far:
            for dx in range(1, groups):
                second.append(("x", d, dx, 0, s))
    for s in range(pieces):
        for d in far:
            for dx in range(1, groups):
                for dy in range(1, planes):
                    last.append(("d", d, dx, dy, s))
    return far, merged + second + last


def kernel(
    lines,
    groups,
    cores,
    planes,
    pieces,
    capacity,
    heads,
    slot_ref,
    request_ref,
    slot_count_ref,
    proj_in,
    src_in,
    dst_in,
    out_weight_ref,
    nodes_ref,
    out_ref,
    where_ref,
    landing_ref,
    table_ref,
    picked_ref,
    z_ref,
    logit_ref,
    count_ref,
    proj_ref,
    src_ref,
    dst_ref,
    local_sems,
    send_sems,
    recv_sems,
    weight_sems,
):
    owned = nodes_ref.shape[1]
    unit = owned // planes
    piece = unit // pieces
    dst_rows = out_ref.shape[0]
    slots = z_ref.shape[0]
    node, y = lax.axis_index("node"), lax.axis_index("head")
    z = node // (groups * cores)
    x = (node // cores) % groups
    c = node % cores

    def device(dz, dx, dc, dy):
        place = (((z + dz) % lines) * groups + (x + dx) % groups) * cores + (c + dc) % cores
        return {"node": place, "head": (y + dy) % planes}

    def number(dz, dx, dc, dy, s):
        place = (((z + dz) % lines) * groups + (x + dx) % groups) * cores + (c + dc) % cores
        return (place * planes + (y + dy) % planes) * pieces + s

    far, events = plan(lines, cores, planes, groups, pieces)
    peers = [(d, 0, 0, 0) for d in far]
    peers += [(0, d, 0, 0) for d in range(1, groups)]
    peers += [(0, 0, d, 0) for d in range(1, cores)]
    peers += [(0, 0, 0, d) for d in range(1, planes)]
    barrier = pltpu.get_barrier_semaphore()
    for peer in peers:
        pl.semaphore_signal(barrier, inc=1, device_id=device(*peer))
    fetch = [
        pltpu.make_async_copy(
            nodes_ref.at[:, pl.ds(k * piece, piece)],
            landing_ref.at[node * planes * pieces + k],
            local_sems.at[3 + k],
        )
        for k in range(planes * pieces)
    ]
    fetch += [
        pltpu.make_async_copy(given, held.at[y], local_sems.at[i])
        for i, (given, held) in enumerate(((proj_in, proj_ref), (src_in, src_ref), (dst_in, dst_ref)))
    ]
    for copy in fetch:
        copy.start()
    pl.semaphore_wait(barrier, len(peers))
    for copy in fetch:
        copy.wait()

    sent = []

    def send(index, peer):
        view = landing_ref.at[index]
        copy = pltpu.make_async_remote_copy(
            src_ref=view,
            dst_ref=view,
            send_sem=send_sems.at[len(sent)],
            recv_sem=recv_sems.at[index],
            device_id=device(*peer),
        )
        copy.start()
        sent.append(copy)

    def landed(index):
        view = landing_ref.at[index]
        pltpu.make_async_remote_copy(
            src_ref=view,
            dst_ref=view,
            send_sem=send_sems.at[0],
            recv_sem=recv_sems.at[index],
            device_id=device(*peers[0]),
        ).wait_recv()

    block = math.gcd(piece, 256)
    eye = (
        lax.broadcasted_iota(jnp.int32, (block, block), 0)
        == lax.broadcasted_iota(jnp.int32, (block, block), 1)
    ).astype(jnp.bfloat16)

    def widen(index):
        for first in range(0, piece, block):
            rows = pl.ds(pl.multiple_of(index * piece + first, block), block)
            table_ref[rows, :] = lax.dot_general(
                eye,
                landing_ref[index, :, first : first + block],
                (((1,), (1,)), ((), ())),
                preferred_element_type=jnp.float32,
            )

    for s in range(pieces):
        for d in far:
            send(number(0, 0, 0, 0, s), (d, 0, 0, 0))
    for dy in range(planes):
        for s in range(pieces):
            for dx in range(1, groups):
                send(number(0, 0, 0, dy, s), (0, dx, 0, 0))
    shared = []
    for i, held in enumerate((proj_ref, src_ref, dst_ref)):
        for dy in range(1, planes):
            copy = pltpu.make_async_remote_copy(
                src_ref=held.at[y],
                dst_ref=held.at[y],
                send_sem=weight_sems.at[0, i, dy],
                recv_sem=weight_sems.at[1, i, dy],
                device_id=device(0, 0, 0, dy),
            )
            copy.start()
            shared.append(copy)
    for dy in range(planes):
        for s in range(pieces):
            for dc in range(1, cores):
                send(number(0, 0, 0, dy, s), (0, 0, dc, 0))

    late = far[:1]
    todo = []
    steps = 16 if dst_rows % 16 == 0 else 1
    share = dst_rows // steps
    base = y * dst_rows

    def catch_up(keep):
        while len(todo) > keep:
            dz, dx, dy, s = todo.pop(0)
            for dc in range(1, cores):
                index = number(dz, dx, dc, dy, s)
                landed(index)
                widen(index)

    for dy in range(planes):
        for s in range(pieces):
            widen(number(0, 0, 0, dy, s))
            todo.append((0, 0, dy, s))
    for e, (kind, dz, dx, dy, s) in enumerate(events):
        if e < steps:
            address_rows(
                e * share, share, base, slots, dst_rows, slot_ref, request_ref, where_ref, owned, capacity
            )
        if e == steps:

            def fill(row, carry):
                count_ref[pl.ds(row, 1), :] = jnp.full((1, LANES), slot_count_ref[base + row])
                return carry

            lax.fori_loop(0, dst_rows, fill, 0)
        index = number(dz, dx, 0, dy, s)
        landed(index)
        if kind == "z":
            for d in range(1, planes):
                send(index, (0, 0, 0, d))
        if kind == "z" or (kind == "y" and dz in late):
            for d in range(1, groups):
                send(index, (0, d, 0, 0))
        if kind == "x" and dz not in late:
            for d in range(1, planes):
                send(index, (0, 0, 0, d))
        for dc in range(1, cores):
            send(index, (0, 0, dc, 0))
        widen(index)
        todo.append((dz, dx, dy, s))
        catch_up(2)
    catch_up(0)
    for copy in sent:
        copy.wait_send()
    for copy in shared:
        copy.wait()
    gather_rows(where_ref, table_ref, picked_ref)
    attend(
        heads, proj_ref, src_ref, dst_ref, count_ref, out_weight_ref, out_ref, picked_ref, z_ref, logit_ref
    )


def local(
    features, proj_weight, score_src, score_dst, request_rows, slot_index, slot_count, out_weight
):
    planes = lax.axis_size("head")
    nodes = lax.axis_size("node")
    owned, feat = features.shape
    capacity = request_rows.shape[2]
    local_heads, head_dim = score_src.shape
    heads = local_heads * planes
    width = proj_weight.shape[1]
    dst_rows = slot_index.shape[0] // planes
    slots = slot_index.shape[1]
    cores = 2 if nodes % 2 == 0 else 1
    chips = nodes // cores
    lines = 4 if chips % 4 == 0 else chips
    groups = chips // lines
    pieces = 2 if planes <= 2 else 1
    units = nodes * planes * pieces
    vmem = pl.BlockSpec(memory_space=pltpu.VMEM)
    smem = pl.BlockSpec(memory_space=pltpu.SMEM)
    anyway = pl.BlockSpec(memory_space=pl.ANY)
    far, events = plan(lines, cores, planes, groups, pieces)
    sends = pieces * (len(far) + planes * (groups - 1) + planes * (cores - 1))
    for kind, dz, _, _, _ in events:
        sends += cores - 1
        if kind == "z":
            sends += planes - 1 + groups - 1
        if kind == "y" and dz in far[:1]:
            sends += groups - 1
        if kind == "x" and dz not in far[:1]:
            sends += planes - 1
    return pl.pallas_call(
        functools.partial(kernel, lines, groups, cores, planes, pieces, capacity, heads),
        out_shape=jax.ShapeDtypeStruct((dst_rows, out_weight.shape[1]), jnp.bfloat16),
        in_specs=[smem, smem, smem, anyway, anyway, anyway, vmem, anyway],
        out_specs=vmem,
        scratch_shapes=[
            pltpu.SMEM((dst_rows * slots,), jnp.int32),
            pltpu.VMEM((units, feat, owned // planes // pieces), jnp.bfloat16),
            pltpu.VMEM((nodes * owned, feat), jnp.float32),
            pltpu.VMEM((dst_rows * slots, feat), jnp.float32),
            pltpu.VMEM((slots, dst_rows, width * planes), jnp.bfloat16),
            pltpu.VMEM((slots, dst_rows, LANES), jnp.float32),
            pltpu.VMEM((dst_rows, LANES), jnp.int32),
            pltpu.VMEM((planes, feat, width), jnp.bfloat16),
            pltpu.VMEM((planes, local_heads, head_dim), jnp.float32),
            pltpu.VMEM((planes, local_heads, head_dim), jnp.float32),
            pltpu.SemaphoreType.DMA((3 + planes * pieces,)),
            pltpu.SemaphoreType.DMA((sends,)),
            pltpu.SemaphoreType.DMA((units,)),
            pltpu.SemaphoreType.DMA((2, 3, planes)),
        ],
        compiler_params=pltpu.CompilerParams(
            vmem_limit_bytes=67043328, collective_id=0, has_side_effects=True
        ),
    )(slot_index.T, request_rows, slot_count, proj_weight, score_src, score_dst, out_weight, features.T)


def solution(mesh):
    in_specs = (
        P("node", None),
        P(None, "head"),
        P("head", None),
        P("head", None),
        P("node", None, None),
        P("node", None),
        P("node"),
        P(),
    )
    out_specs = P(("node", "head"), None)
    return jax.shard_map(local, mesh=mesh, in_specs=in_specs, out_specs=out_specs, check_vma=False)
```
